32 devices in a mesh: atom: 8 (over z, x), energy: 4 (over y, core).
Axes of the slice: x: 2, y: 2, z: 4, core: 2. Of those that a mesh axis runs over, the one named last changes fastest.
Arguments:
- t_matrix: float32 [4, 64, 16, 16], P('energy', 'atom'), may hold values from -1.5 to 1.5
- structure: bfloat16 [4, 64, 1024, 1024], P('energy', 'atom'), may hold values from -0.125 to 0.125
- radial: bfloat16 [4, 64, 16, 1024], P('energy', 'atom'), may hold values from -3 to 3
- weights: float32 [4], P('energy'), may hold values from 0.1 to 1
- neighbours: int32 [64, 64], P('atom'), may hold values from 0 to 63, as said below
- live: int32 [64, 64], P('atom'), may hold values from 0 to 1, as said below
Outputs:
- density: float32 [64, 1024], P('atom', 'energy')
The draws below stay inside these ranges and needn't reach their ends.
Inputs may be any that keep to these rules, and one draw needn't show every extreme that they name: `neighbours`: slot 0 of atom i holds i itself. Atom i lies at index i // 8 of the atom axis, and every neighbour of it lies at an index that differs from that one by at most 3 around the axis, which closes into a loop; both extremes occur in every draw. An atom may appear in several slots of one zone. `live`: each row is 1 on its first slots and 0 after; slot 0 is always 1, at least 16 slots are 1, and some atom has all 64 slots 1.
All inputs are finite; a program needn't handle non-finite values.
Results may differ from the reference program's by a relative error of at most 0.0043.
Values sent between devices are 32-bit elements; how exact they have to be, the bound alone decides.
A program may use at most 128 MiB of HBM per device.

```python
import math
import jax
import jax.numpy as jnp
from jax import lax

LM = 16
NB = 64
R = 1024
ITERS = 4
SPAN = 3
A_DEV = 8
ATOMS = 64
ENERGIES = 4


def draw_neighbours(key, part):
    first_key, second_key = jax.random.split(jax.random.fold_in(key, 11))
    n_devices = ATOMS // A_DEV
    owner = jnp.arange(ATOMS, dtype=jnp.int32) // A_DEV
    offsets = jax.random.randint(first_key, (ATOMS, NB), -SPAN, SPAN + 1)
    offsets = offsets.at[:, 1].set(SPAN).at[:, 2].set(-SPAN)
    slots = jax.random.randint(second_key, (ATOMS, NB), 0, A_DEV)
    device = (owner[:, None] + offsets + n_devices) % n_devices
    picked = device * A_DEV + slots
    picked = picked.at[:, 0].set(jnp.arange(ATOMS, dtype=jnp.int32))
    return picked.astype(jnp.int32)


def draw_live(key, part):
    counts = jax.random.randint(jax.random.fold_in(key, 23), (ATOMS,), NB // 4, NB + 1)
    counts = counts.at[0].set(NB)
    return (jnp.arange(NB)[None, :] < counts[:, None]).astype(jnp.int32)


def block_levels(rng, shape, pieces, smallest, top_value):
    gain, own = 1.0, jax.random.fold_in(rng, 6)
    for axis_at, blocks in pieces:
        draws = jnp.exp(jax.random.uniform(jax.random.fold_in(own, axis_at), (blocks,), jnp.float32, smallest / len(pieces), top_value / len(pieces)))
        gain = gain * jnp.repeat(draws, shape[axis_at] // blocks).reshape([-1 if axis == axis_at else 1 for axis in range(len(shape))])
    return gain


def bell_draw(key, shape, deviation, most, cuts=(), kind=jnp.bfloat16):
    loudness = block_levels(key, shape, cuts, -0.22, 0.18) if cuts else 1.0
    drawn = jax.random.normal(key, shape, jnp.float32) * deviation * loudness
    return jnp.minimum(jnp.maximum(drawn, -most), most).astype(kind)


def setup_inputs(seed: int = 0) -> dict:
    splits = jax.random.split(jax.random.key(seed), 7)
    return {
        "t_matrix": bell_draw(splits[0], (ENERGIES, ATOMS, LM, LM), LM ** -0.5, 1.5, ((0, 4), (1, 8)), jnp.float32),
        "structure": bell_draw(splits[1], (ENERGIES, ATOMS, NB * LM, NB * LM), (2 * NB * LM) ** -0.5, 0.125, ((0, 4), (1, 8))),
        "radial": bell_draw(splits[2], (ENERGIES, ATOMS, LM, R), 0.5, 3.0, ((0, 4), (1, 8))),
        "weights": jnp.clip(jnp.exp(math.log(1.0) - 2.3025851 * jax.random.uniform(splits[3], (ENERGIES,), jnp.float32) ** block_levels(splits[3], (ENERGIES,), ((0, 4),), -0.2, 0.2)), 0.1, 1.0),
        "neighbours": draw_neighbours(jax.random.fold_in(splits[6], 71), 0),
        "live": draw_live(jax.random.fold_in(splits[6], 71), 0),
    }


def zone_column(args):
    t_self, g_here, zt_here = args
    rest = jnp.zeros((NB - 1, LM, LM), jnp.float32)
    first = jnp.concatenate([t_self[None], rest], axis=0)
    g_float = g_here.astype(jnp.float32)
    zt_float = zt_here.astype(jnp.float32)
    column = first
    for step in range(ITERS):
        flat_b = lax.optimization_barrier(column.astype(jnp.bfloat16))
        flat = flat_b.astype(jnp.float32).reshape(NB * LM, LM)
        image = jnp.dot(g_float, flat, precision=lax.Precision.HIGHEST)
        image_b = lax.optimization_barrier(image.astype(jnp.bfloat16))
        image_f = image_b.astype(jnp.float32).reshape(NB, LM, LM)
        column = first + jnp.einsum("sij,sjk->sik", zt_float, image_f, precision=lax.Precision.HIGHEST)
    return column


def reference(t_matrix, structure, radial, weights, neighbours, live):
    live_f = live.astype(jnp.float32)
    flat_ids = neighbours.reshape(-1)

    def per_energy(args):
        t_here, g_here, z_here = args
        zone_t = (t_here[neighbours] * live_f[:, :, None, None]).astype(jnp.bfloat16)
        column = lax.map(zone_column, (t_here, g_here, zone_t))
        blocks = (column * live_f[:, :, None, None]).reshape(ATOMS * NB, LM, LM)
        received = jax.ops.segment_sum(blocks, flat_ids, num_segments=ATOMS)
        received_b = lax.optimization_barrier(received.astype(jnp.bfloat16))
        z_float = z_here.astype(jnp.float32)
        turned = jnp.einsum("alm,amr->alr", received_b.astype(jnp.float32), z_float, precision=lax.Precision.HIGHEST)
        return jnp.sum(z_float * turned, axis=1)

    partial_value = lax.map(per_energy, (t_matrix, structure, radial))
    return jnp.sum(weights[:, None, None] * partial_value, axis=0)
```

```python
import functools

import jax
import jax.numpy as jnp
from jax import lax
from jax.experimental import pallas as pl
from jax.experimental.pallas import tpu as pltpu
from jax.sharding import PartitionSpec as P

ITERS = 4
SPAN = 3

NT = (((1,), (1,)), ((), ()))
NN = (((1,), (0,)), ((), ()))


def mm(a, b, dims=NN):
    return lax.dot_general(a, b, dims, preferred_element_type=jnp.float32)


WAIT = 300


def in_order(jobs):
    users = {name: [] for name in jobs}
    for name, (_, deps, _) in jobs.items():
        for dep in deps:
            users[dep].append(name)
    rank = {}

    def rank_of(name):
        if name not in rank:
            rank[name] = jobs[name][0] + max((WAIT + rank_of(user) for user in users[name]), default=0)
        return rank[name]

    order, ready_at, clock = [], {name: 0 for name in jobs if not jobs[name][1]}, 0
    missing = {name: len(deps) for name, (_, deps, _) in jobs.items()}
    at = {name: 0 for name in jobs}
    while ready_at:
        now = [name for name, t in ready_at.items() if t <= clock]
        if not now:
            clock = min(ready_at.values())
            continue
        name = max(now, key=rank_of)
        del ready_at[name]
        clock += jobs[name][0]
        order.append(jobs[name][2])
        for user in users[name]:
            at[user] = max(at[user], clock + WAIT)
            missing[user] -= 1
            if missing[user] == 0:
                ready_at[user] = at[user]
    return order


def kernel(
    n_atom, n_energy, a_dev, lm, zone,
    t_hbm, s_hbm, r_hbm, w_hbm, nb_hbm, live_hbm, out_ref,
    t_ref, w_ref, nb_ref, live_ref, s_v, s_t, r_v, t_send, t_all, firstx, table, hot, bd, pick, mask, reach, x12, x3, v, v3, v4,
    idx_v, idx_s, acc, landed, d_mine, d_land,
    s_sem, misc_sem, ts_sem, tr_sem, as_sem, ar_sem, ds_sem, dr_sem,
):
    bf16, f32 = jnp.bfloat16, jnp.float32
    places = 2 * SPAN + 1
    lanes = a_dev * lm
    dim = zone * lm
    per = lanes // lm
    me = lax.axis_index("atom")
    my_e = lax.axis_index("energy")

    small = [
        pltpu.make_async_copy(source, target, misc_sem.at[2 + n])
        for n, (source, target) in enumerate(
            ((t_hbm, t_ref), (nb_hbm, nb_ref), (live_hbm, live_ref), (w_hbm, w_ref))
        )
    ]
    for copy in small:
        copy.start()
    tile = min(256, dim)
    blocks = dim // tile
    s_copies = [pltpu.make_async_copy(s_hbm.at[a], s_v.at[a], s_sem.at[a]) for a in range(a_dev)]
    for copy in s_copies:
        copy.start(priority=1)
    r_copy = pltpu.make_async_copy(r_hbm, r_v, misc_sem.at[0])
    r_copy.start(priority=1)

    def atom_at(d):
        return lax.rem(me + (d + n_atom), n_atom)

    shifts = [s * d for d in range(SPAN, 0, -1) for s in (-1, 1)]
    barrier = pltpu.get_barrier_semaphore()
    for d in shifts:
        pl.semaphore_signal(barrier, inc=1, device_id={"atom": atom_at(d)}, device_id_type=pl.DeviceIdType.MESH)
    for d in range(1, n_energy):
        pl.semaphore_signal(
            barrier, inc=1, device_id={"energy": lax.rem(my_e + d, n_energy)}, device_id_type=pl.DeviceIdType.MESH
        )

    for copy in small:
        copy.wait()
    t_turned = jnp.transpose(t_ref[...])
    t_send[...] = t_turned
    ids = nb_ref[...] - (me - SPAN) * a_dev
    total = n_atom * a_dev
    ids = jnp.where(ids < 0, ids + total, ids)
    ids = jnp.where(ids >= total, ids - total, ids)
    ids = jnp.where(live_ref[...] > 0, ids, places * a_dev)
    idx_v[...] = ids
    i_copy = pltpu.make_async_copy(idx_v, idx_s, misc_sem.at[1])
    i_copy.start()

    lane16 = lax.broadcasted_iota(jnp.int32, (lm, lanes), 1)
    row16 = lax.broadcasted_iota(jnp.int32, (lm, lanes), 0)
    for a in range(a_dev):
        moved = t_turned if a == 0 else pltpu.roll(t_turned, lanes - a * lm, 1)
        firstx[a] = jnp.where(lane16 < lm, moved, 0.0)

    place_of = jnp.zeros(ids.shape, f32)
    for p in range(1, places + 1):
        place_of = place_of + jnp.where(ids >= p * a_dev, 1.0, 0.0)
    wide = lax.broadcasted_iota(jnp.int32, (zone, dim), 1)
    tall = lax.broadcasted_iota(jnp.int32, (zone, dim), 0)
    widen = jnp.where((wide >= tall * lm) & (wide < tall * lm + lm), 1.0, 0.0).astype(bf16)
    spread_place = mm(place_of.astype(bf16), widen)
    for a in range(a_dev):
        reach[a] = jnp.broadcast_to(spread_place[a:a + 1], (lm, dim))

    for n in range(a_dev):
        one = jnp.where(lane16 - row16 == n * lm, 1.0, 0.0).astype(bf16)
        for p in range(places):
            hot[p * a_dev + n] = one
    hot[places * a_dev] = jnp.zeros((lm, lanes), bf16)

    row = lax.broadcasted_iota(jnp.int32, (lanes, lanes), 0)
    col = lax.broadcasted_iota(jnp.int32, (lanes, lanes), 1)
    row_block, col_block = row // lm, col // lm
    same = row_block == col_block
    spread = jnp.where(row - row_block * lm == col - col_block * lm, 1.0, 0.0).astype(bf16)

    def diagonal(block):
        return jnp.where(same, jnp.concatenate([block] * a_dev, axis=0), 0.0).astype(bf16)

    unit = lax.broadcasted_iota(jnp.int32, (tile, tile), 0) == lax.broadcasted_iota(jnp.int32, (tile, tile), 1)
    unit = jnp.where(unit, 1.0, 0.0).astype(bf16)
    start = jnp.zeros((lm, tile - lanes), f32)

    def left_of(a, c):
        if c > 0:
            return unit
        return jnp.concatenate([unit, jnp.concatenate([firstx[a], start], axis=1).astype(bf16)], axis=0)

    def turn_tile(a, c, rows):
        got = mm(left_of(a, c), s_v[a, rows, c * tile:(c + 1) * tile], NT).astype(bf16)
        s_t[a, c * tile:(c + 1) * tile, rows] = got[:tile]
        if c == 0:
            v[a, :, rows] = got[tile:]

    def fill_pick(a):
        for s in range(zone):
            pick[a, pl.ds(s * lm, lm), :] = hot[idx_s[a, s]]

    def turn(a, carry):
        pltpu.make_async_copy(s_hbm.at[a], s_v.at[a], s_sem.at[a]).wait()
        for c in range(blocks):
            turn_tile(a, c, slice(0, dim))
        for p in range(places):
            mask[a, p] = jnp.where(reach[a] == p, 1.0, 0.0).astype(bf16)
        return carry

    early = a_dev * 3 // 8
    lax.fori_loop(0, early, turn, 0)

    pl.semaphore_wait(barrier, len(shifts) + n_energy - 1)

    def send_t(d):
        return pltpu.make_async_remote_copy(
            src_ref=t_send, dst_ref=t_all.at[SPAN - d], send_sem=ts_sem.at[SPAN - d],
            recv_sem=tr_sem.at[SPAN - d], device_id={"atom": atom_at(d)}, device_id_type=pl.DeviceIdType.MESH,
        )

    t_copies = [send_t(d) for d in shifts]
    for copy in t_copies:
        copy.start()

    lax.fori_loop(early, a_dev, turn, 0)
    i_copy.wait()

    def fill_table(place, block):
        block = mm(diagonal(block), spread).astype(bf16)
        table[pl.ds(place * a_dev, a_dev)] = block.reshape(a_dev, lm, lanes)

    fill_table(SPAN, t_turned)
    table[places * a_dev] = jnp.zeros((lm, lanes), bf16)
    for copy in t_copies:
        copy.wait()
    for d in shifts:
        fill_table(SPAN - d, t_all[SPAN - d])

    keep = [jnp.where(lane16 // lm == b, 1.0, 0.0).astype(bf16) for b in range(per)]

    def fill_bd(a):
        for s in range(zone):
            bd[a, pl.ds(s * lm, lm), :] = table[idx_s[a, s]] * keep[s % per]

    def column(a, r):
        parts = []
        for g in range(r * tile // lanes, (r + 1) * tile // lanes):
            at = slice(g * lanes, (g + 1) * lanes)
            part = mm(v[a, :, at], bd[a, at, :])
            if g == 0:
                part = part + firstx[a]
            parts.append(part.astype(bf16))
        return jnp.concatenate(parts, axis=1)

    def cols(lo, hi):
        return slice(lo * tile, hi * tile)

    def start_columns(a):
        for r in range(blocks):
            x12[a, :lm, cols(r, r + 1)] = column(a, r)

    def sweep_a(a, r):
        here = cols(r, r + 1)
        got = mm(x12[a, :lm, cols(r, blocks)], s_t[a, cols(r, blocks), here])
        if r > 0:
            both = mm(x12[a, :, cols(0, r)], s_t[a, cols(0, r), here])
            got = got + both[:lm]
            v3[a, :, here] = both[lm:]
        v[a, :, here] = got.astype(bf16)

    def column_a(a, r):
        got = column(a, r)
        x12[a, lm:, cols(r, r + 1)] = got
        x3[a, :lm, cols(r, r + 1)] = got

    def sweep_b(a, r):
        here = cols(r, r + 1)
        got = mm(x3[a, :lm, cols(r, r + 1)], s_t[a, here, here])
        if r + 1 < blocks:
            both = mm(x3[a, :, cols(r + 1, blocks)], s_t[a, cols(r + 1, blocks), here])
            got = got + both[:lm]
            v4[a, :, here] = both[lm:]
        if r > 0:
            got = got + v3[a, :, here]
        v[a, :, here] = got.astype(bf16)

    def column_b(a, r):
        x3[a, lm:, cols(r, r + 1)] = column(a, r)

    def sweep_c(a, r):
        here = cols(r, r + 1)
        got = mm(x3[a, lm:, cols(0, r + 1)], s_t[a, cols(0, r + 1), here])
        if r + 1 < blocks:
            got = got + v4[a, :, here]
        v[a, :, here] = got.astype(bf16)

    whole = [None]

    def scatter(a, r):
        here = cols(r, r + 1)
        block = v[a, :, here]
        left = jnp.concatenate([block * mask[a, p, :, here] for p in range(places)], axis=0)
        got = mm(left, pick[a, here, :])
        whole[0] = got if whole[0] is None else whole[0] + got

    step = tile // 8
    jobs = {}

    def job(name, cost, deps, fn, *args):
        jobs[name] = (cost, deps, functools.partial(fn, *args))

    for a in range(a_dev):
        job(("f", a), 2 * step, [], fill_bd, a)
        job(("p", a), 0, [("z", a)], fill_pick, a)
        job(("z", a), blocks * step, [("f", a)], start_columns, a)
        for r in range(blocks):
            job(("a", a, r), blocks * step, [("z", a)] + [("ca", a, c) for c in range(r)], sweep_a, a, r)
            job(("ca", a, r), step, [("a", a, r)], column_a, a, r)
            later = range(r + 1, blocks)
            job(("b", a, r), (blocks - r) * step, [("ca", a, r)] + [("cb", a, c) for c in later], sweep_b, a, r)
            job(("cb", a, r), step, [("b", a, r)], column_b, a, r)
            job(("c", a, r), (r + 1) * step, [("cb", a, c) for c in range(r + 1)], sweep_c, a, r)
            job(("s", a, r), step, [("c", a, r), ("p", a)], scatter, a, r)
    for fn in in_order(jobs):
        fn()

    def send_acc(d):
        return pltpu.make_async_remote_copy(
            src_ref=acc.at[SPAN + d], dst_ref=landed.at[SPAN - d], send_sem=as_sem.at[SPAN - d],
            recv_sem=ar_sem.at[SPAN - d], device_id={"atom": atom_at(d)}, device_id_type=pl.DeviceIdType.MESH,
        )

    for p in range(places):
        acc[p] = whole[0][p * lm:(p + 1) * lm]
    a_copies = [send_acc(d) for d in shifts]
    for copy in a_copies:
        copy.start()
    r_copy.wait()
    own = diagonal(t_turned)
    for copy in a_copies:
        copy.wait()
    gathered = acc[SPAN]
    for d in shifts:
        gathered = gathered + landed[SPAN - d]
    high = gathered.astype(bf16)
    low = (gathered - high.astype(f32)).astype(bf16)
    received = t_turned + (mm(high, own) + mm(low, own))
    turned = mm(diagonal(received.astype(bf16).astype(f32)), r_v[...])
    products = turned * r_v[...].astype(f32)
    density = jnp.sum(products.reshape(a_dev, lm, products.shape[1]), axis=1) * w_ref[0]
    share = density.shape[1] // n_energy
    for q in range(n_energy):
        d_mine[q] = density[:, q * share:(q + 1) * share]

    def send_d(d):
        to = lax.rem(my_e + d, n_energy)
        return pltpu.make_async_remote_copy(
            src_ref=d_mine.at[to], dst_ref=d_land.at[d - 1], send_sem=ds_sem.at[d - 1],
            recv_sem=dr_sem.at[d - 1], device_id={"energy": to}, device_id_type=pl.DeviceIdType.MESH,
        )

    d_copies = [send_d(d) for d in range(1, n_energy)]
    for copy in d_copies:
        copy.start()
    for copy in d_copies:
        copy.wait()
    result = d_mine[my_e]
    for d in range(1, n_energy):
        result = result + d_land[d - 1]
    out_ref[...] = result


def shards(n_atom, n_energy, t_matrix, structure, radial, weights, neighbours, live):
    _, a_dev, lm, _ = t_matrix.shape
    zone = neighbours.shape[1]
    mesh_points = radial.shape[-1]
    dim, lanes, places = zone * lm, a_dev * lm, 2 * SPAN + 1
    share = mesh_points // n_energy
    vmem = pl.BlockSpec(memory_space=pltpu.VMEM)
    hbm = pl.BlockSpec(memory_space=pltpu.HBM)
    f32, bf16 = jnp.float32, jnp.bfloat16
    dma = pltpu.SemaphoreType.DMA
    pin = functools.partial(pltpu.with_memory_space_constraint, memory_space=pltpu.HBM)
    return pl.pallas_call(
        functools.partial(kernel, n_atom, n_energy, a_dev, lm, zone),
        out_shape=jax.ShapeDtypeStruct((a_dev, share), f32),
        in_specs=[hbm] * 6,
        out_specs=vmem,
        scratch_shapes=[
            pltpu.VMEM((lanes, lm), f32),
            pltpu.SMEM((1,), f32),
            pltpu.VMEM((a_dev, zone), jnp.int32),
            pltpu.VMEM((a_dev, zone), jnp.int32),
            pltpu.VMEM((a_dev, dim, dim), bf16),
            pltpu.VMEM((a_dev, dim, dim), bf16),
            pltpu.VMEM((lanes, mesh_points), bf16),
            pltpu.VMEM((lm, lanes), f32),
            pltpu.VMEM((places, lm, lanes), f32),
            pltpu.VMEM((a_dev, lm, lanes), f32),
            pltpu.VMEM((places * a_dev + 1, lm, lanes), bf16),
            pltpu.VMEM((places * a_dev + 1, lm, lanes), bf16),
            pltpu.VMEM((a_dev, dim, lanes), bf16),
            pltpu.VMEM((a_dev, dim, lanes), bf16),
            pltpu.VMEM((a_dev, places, lm, dim), bf16),
            pltpu.VMEM((a_dev, lm, dim), f32),
            pltpu.VMEM((a_dev, 2 * lm, dim), bf16),
            pltpu.VMEM((a_dev, 2 * lm, dim), bf16),
            pltpu.VMEM((a_dev, lm, dim), bf16),
            pltpu.VMEM((a_dev, lm, dim), f32),
            pltpu.VMEM((a_dev, lm, dim), f32),
            pltpu.VMEM((a_dev, zone), jnp.int32),
            pltpu.SMEM((a_dev, zone), jnp.int32),
            pltpu.VMEM((places, lm, lanes), f32),
            pltpu.VMEM((places, lm, lanes), f32),
            pltpu.VMEM((n_energy, a_dev, share), f32),
            pltpu.VMEM((n_energy, a_dev, share), f32),
            dma((a_dev,)),
            dma((6,)),
            dma((places,)),
            dma((places,)),
            dma((places,)),
            dma((places,)),
            dma((n_energy,)),
            dma((n_energy,)),
        ],
        compiler_params=pltpu.CompilerParams(collective_id=0, has_side_effects=True, vmem_limit_bytes=52 * 1024 * 1024),
        name="tau_density",
    )(
        pin(t_matrix.reshape(lanes, lm)),
        pin(structure.reshape(a_dev, dim, dim)),
        pin(radial.reshape(lanes, mesh_points)),
        weights,
        pin(neighbours),
        pin(live),
    )


def solution(mesh):
    in_specs = (
        P("energy", "atom", None, None),
        P("energy", "atom", None, None),
        P("energy", "atom", None, None),
        P("energy"),
        P("atom", None),
        P("atom", None),
    )
    out_specs = P("atom", "energy")
    body = functools.partial(shards, mesh.shape["atom"], mesh.shape["energy"])
    return jax.shard_map(body, mesh=mesh, in_specs=in_specs, out_specs=out_specs, check_vma=False)
```

```python
import functools

import jax
import jax.numpy as jnp
from jax import lax
from jax.experimental import pallas as pl
from jax.experimental.pallas import tpu as pltpu
from jax.sharding import PartitionSpec as P

ITERS = 4
SPAN = 3

NT = (((1,), (1,)), ((), ()))
NN = (((1,), (0,)), ((), ()))


def mm(a, b, dims=NN):
    return lax.dot_general(a, b, dims, preferred_element_type=jnp.float32)


WAIT = 300


def in_order(jobs):
    users = {name: [] for name in jobs}
    for name, (_, deps, _) in jobs.items():
        for dep in deps:
            users[dep].append(name)
    rank = {}

    def rank_of(name):
        if name not in rank:
            rank[name] = jobs[name][0] + max((WAIT + rank_of(user) for user in users[name]), default=0)
        return rank[name]

    order, ready_at, clock = [], {name: 0 for name in jobs if not jobs[name][1]}, 0
    missing = {name: len(deps) for name, (_, deps, _) in jobs.items()}
    at = {name: 0 for name in jobs}
    while ready_at:
        now = [name for name, t in ready_at.items() if t <= clock]
        if not now:
            clock = min(ready_at.values())
            continue
        name = max(now, key=rank_of)
        del ready_at[name]
        clock += jobs[name][0]
        order.append(jobs[name][2])
        for user in users[name]:
            at[user] = max(at[user], clock + WAIT)
            missing[user] -= 1
            if missing[user] == 0:
                ready_at[user] = at[user]
    return order


def kernel(
    n_atom, n_energy, a_dev, lm, zone,
    t_hbm, s_hbm, r_hbm, w_hbm, nb_hbm, live_hbm, out_ref,
    t_ref, w_ref, nb_ref, live_ref, s_v, s_t, r_v, t_send, t_all, firstx, table, hot, bd, pick, mask, reach, x12, x3, v, v3, v4, share,
    idx_v, idx_s, acc, landed, d_mine, d_land,
    s_sem, misc_sem, ts_sem, tr_sem, as_sem, ar_sem, ds_sem, dr_sem,
):
    bf16, f32 = jnp.bfloat16, jnp.float32
    places = 2 * SPAN + 1
    lanes = a_dev * lm
    dim = zone * lm
    per = lanes // lm
    me = lax.axis_index("atom")
    my_e = lax.axis_index("energy")

    small = [
        pltpu.make_async_copy(source, target, misc_sem.at[2 + n])
        for n, (source, target) in enumerate(
            ((t_hbm, t_ref), (nb_hbm, nb_ref), (live_hbm, live_ref), (w_hbm, w_ref))
        )
    ]
    for copy in small:
        copy.start()
    tile = min(256, dim)
    blocks = dim // tile
    s_copies = [pltpu.make_async_copy(s_hbm.at[a], s_v.at[a], s_sem.at[a]) for a in range(a_dev)]
    for copy in s_copies:
        copy.start(priority=1)
    r_copy = pltpu.make_async_copy(r_hbm, r_v, misc_sem.at[0])
    r_copy.start(priority=1)

    def atom_at(d):
        return lax.rem(me + (d + n_atom), n_atom)

    shifts = [s * d for d in range(SPAN, 0, -1) for s in (-1, 1)]
    barrier = pltpu.get_barrier_semaphore()
    for d in shifts:
        pl.semaphore_signal(barrier, inc=1, device_id={"atom": atom_at(d)}, device_id_type=pl.DeviceIdType.MESH)
    for d in range(1, n_energy):
        pl.semaphore_signal(
            barrier, inc=1, device_id={"energy": lax.rem(my_e + d, n_energy)}, device_id_type=pl.DeviceIdType.MESH
        )

    for copy in small:
        copy.wait()
    t_turned = jnp.transpose(t_ref[...])
    t_send[...] = t_turned
    ids = nb_ref[...] - (me - SPAN) * a_dev
    total = n_atom * a_dev
    ids = jnp.where(ids < 0, ids + total, ids)
    ids = jnp.where(ids >= total, ids - total, ids)
    ids = jnp.where(live_ref[...] > 0, ids, places * a_dev)
    idx_v[...] = ids
    i_copy = pltpu.make_async_copy(idx_v, idx_s, misc_sem.at[1])
    i_copy.start()

    lane16 = lax.broadcasted_iota(jnp.int32, (lm, lanes), 1)
    row16 = lax.broadcasted_iota(jnp.int32, (lm, lanes), 0)
    for a in range(a_dev):
        moved = t_turned if a == 0 else pltpu.roll(t_turned, lanes - a * lm, 1)
        firstx[a] = jnp.where(lane16 < lm, moved, 0.0)

    place_of = jnp.zeros(ids.shape, f32)
    for p in range(1, places + 1):
        place_of = place_of + jnp.where(ids >= p * a_dev, 1.0, 0.0)
    wide = lax.broadcasted_iota(jnp.int32, (zone, dim), 1)
    tall = lax.broadcasted_iota(jnp.int32, (zone, dim), 0)
    widen = jnp.where((wide >= tall * lm) & (wide < tall * lm + lm), 1.0, 0.0).astype(bf16)
    spread_place = mm(place_of.astype(bf16), widen)
    for a in range(a_dev):
        reach[a] = jnp.broadcast_to(spread_place[a:a + 1], (lm, dim))

    for n in range(a_dev):
        one = jnp.where(lane16 - row16 == n * lm, 1.0, 0.0).astype(bf16)
        for p in range(places):
            hot[p * a_dev + n] = one
    hot[places * a_dev] = jnp.zeros((lm, lanes), bf16)

    row = lax.broadcasted_iota(jnp.int32, (lanes, lanes), 0)
    col = lax.broadcasted_iota(jnp.int32, (lanes, lanes), 1)
    row_block, col_block = row // lm, col // lm
    same = row_block == col_block
    spread = jnp.where(row - row_block * lm == col - col_block * lm, 1.0, 0.0).astype(bf16)

    def diagonal(block):
        return jnp.where(same, jnp.concatenate([block] * a_dev, axis=0), 0.0).astype(bf16)

    unit = lax.broadcasted_iota(jnp.int32, (tile, tile), 0) == lax.broadcasted_iota(jnp.int32, (tile, tile), 1)
    unit = jnp.where(unit, 1.0, 0.0).astype(bf16)
    start = jnp.zeros((lm, tile - lanes), f32)

    def left_of(a, c):
        if c > 0:
            return unit
        return jnp.concatenate([unit, jnp.concatenate([firstx[a], start], axis=1).astype(bf16)], axis=0)

    def turn_tile(a, c, rows):
        got = mm(left_of(a, c), s_v[a, rows, c * tile:(c + 1) * tile], NT).astype(bf16)
        s_t[a, c * tile:(c + 1) * tile, rows] = got[:tile]
        if c == 0:
            v[a, :, rows] = got[tile:]

    def fill_pick(a):
        for s in range(zone):
            pick[a, pl.ds(s * lm, lm), :] = hot[idx_s[a, s]]

    def turn(a, carry):
        pltpu.make_async_copy(s_hbm.at[a], s_v.at[a], s_sem.at[a]).wait()
        for c in range(blocks):
            turn_tile(a, c, slice(0, dim))
        for p in range(places):
            mask[a, p] = jnp.where(reach[a] == p, 1.0, 0.0).astype(bf16)
        return carry

    early = a_dev // 4
    turned_first = a_dev - a_dev * 3 // 8
    lax.fori_loop(0, early, turn, 0)

    pl.semaphore_wait(barrier, len(shifts) + n_energy - 1)

    def send_t(d):
        return pltpu.make_async_remote_copy(
            src_ref=t_send, dst_ref=t_all.at[SPAN - d], send_sem=ts_sem.at[SPAN - d],
            recv_sem=tr_sem.at[SPAN - d], device_id={"atom": atom_at(d)}, device_id_type=pl.DeviceIdType.MESH,
        )

    t_copies = [send_t(d) for d in shifts]
    for copy in t_copies:
        copy.start()

    def begin(a, carry):
        pltpu.make_async_copy(s_hbm.at[a], s_v.at[a], s_sem.at[a]).wait()
        got = mm(firstx[a].astype(bf16), s_v[a, :, :lanes], NT)
        v4[a] = got
        v[a] = got.astype(bf16)
        for p in range(places):
            mask[a, p] = jnp.where(reach[a] == p, 1.0, 0.0).astype(bf16)
        return carry

    lax.fori_loop(early, turned_first, turn, 0)
    lax.fori_loop(turned_first, a_dev, begin, 0)
    i_copy.wait()

    def fill_table(place, block):
        block = mm(diagonal(block), spread).astype(bf16)
        table[pl.ds(place * a_dev, a_dev)] = block.reshape(a_dev, lm, lanes)

    fill_table(SPAN, t_turned)
    table[places * a_dev] = jnp.zeros((lm, lanes), bf16)
    for copy in t_copies:
        copy.wait()
    for d in shifts:
        fill_table(SPAN - d, t_all[SPAN - d])

    keep = [jnp.where(lane16 // lm == b, 1.0, 0.0).astype(bf16) for b in range(per)]

    def fill_bd(a):
        for s in range(zone):
            g = s // per
            at = g // 2 * lanes + s % per * lm
            half = slice(g % 2 * lanes, (g % 2 + 1) * lanes)
            bd[a, at:at + lm, half] = table[idx_s[a, s]] * keep[s % per]

    def column(a, r):
        halves = [slice(h * lanes, (h + 1) * lanes) for h in range(2)]
        left = jnp.concatenate([v[a, :, r * tile + h * lanes:r * tile + (h + 1) * lanes] for h in range(2)], axis=0)
        both = mm(left, bd[a, r * lanes:(r + 1) * lanes, :])
        parts = [both[h * lm:(h + 1) * lm, halves[h]] for h in range(2)]
        if r == 0:
            parts[0] = parts[0] + firstx[a]
        return jnp.concatenate([part.astype(bf16) for part in parts], axis=1)

    def cols(lo, hi):
        return slice(lo * tile, hi * tile)

    def start_columns(a):
        for r in range(blocks):
            x12[a, :lm, cols(r, r + 1)] = column(a, r)

    def sweep_a(a, r):
        here = cols(r, r + 1)
        got = mm(x12[a, :lm, cols(r, blocks)], s_t[a, cols(r, blocks), here])
        if r > 0:
            both = mm(x12[a, :, cols(0, r)], s_t[a, cols(0, r), here])
            got = got + both[:lm]
            v3[a, :, here] = both[lm:]
        v[a, :, here] = got.astype(bf16)

    def column_a(a, r):
        got = column(a, r)
        x12[a, lm:, cols(r, r + 1)] = got
        x3[a, :lm, cols(r, r + 1)] = got

    def sweep_b(a, r):
        here = cols(r, r + 1)
        got = mm(x3[a, :lm, cols(r, r + 1)], s_t[a, here, here])
        if r + 1 < blocks:
            both = mm(x3[a, :, cols(r + 1, blocks)], s_t[a, cols(r + 1, blocks), here])
            got = got + both[:lm]
            v4[a, :, here] = both[lm:]
        if r > 0:
            got = got + v3[a, :, here]
        v[a, :, here] = got.astype(bf16)

    def column_b(a, r):
        x3[a, lm:, cols(r, r + 1)] = column(a, r)

    def sweep_c(a, r):
        here = cols(r, r + 1)
        got = mm(x3[a, lm:, cols(0, r + 1)], s_t[a, cols(0, r + 1), here])
        if r + 1 < blocks:
            got = got + v4[a, :, here]
        v[a, :, here] = got.astype(bf16)

    void = jnp.zeros((lanes, lanes), bf16)

    def fold(a, c):
        rows = []
        for g in range(2):
            block = bd[a, c * lanes:(c + 1) * lanes, g * lanes:(g + 1) * lanes]
            rows.append(jnp.concatenate([block, void] if g == 0 else [void, block], axis=1))
        left = jnp.concatenate(rows + [x12[a, :lm, cols(c, c + 1)]], axis=0)
        got = mm(left, s_v[a, :, cols(c, c + 1)], NT)
        s_t[a, cols(c, c + 1), :] = got[:tile].astype(bf16)
        share[a - turned_first, c] = got[tile:]

    def gather(a):
        got = share[a - turned_first, 0]
        for c in range(1, blocks):
            got = got + share[a - turned_first, c]
        x12[a, :lm, :] = got.astype(bf16)

    def fold_a(a, r):
        here = cols(r, r + 1)
        got = mm(x12[a, :lm, cols(r, blocks)], s_t[a, cols(r, blocks), here]) + v4[a, :, here]
        if r > 0:
            both = mm(x12[a, :, cols(0, r)], s_t[a, cols(0, r), here])
            got = got + both[:lm]
            v3[a, :, here] = both[lm:]
        x12[a, lm:, here] = got.astype(bf16)
        x3[a, :lm, here] = got.astype(bf16)

    def fold_b(a, r):
        here = cols(r, r + 1)
        got = mm(x3[a, :lm, cols(r, blocks)], s_t[a, cols(r, blocks), here]) + v4[a, :, here]
        if r > 0:
            got = got + v3[a, :, here]
        v[a, :, here] = got.astype(bf16)

    whole = [None]

    def scatter(a, r):
        here = cols(r, r + 1)
        block = v[a, :, here]
        left = jnp.concatenate([block * mask[a, p, :, here] for p in range(places)], axis=0)
        got = mm(left, pick[a, here, :])
        whole[0] = got if whole[0] is None else whole[0] + got

    step = tile // 8
    jobs = {}

    def job(name, cost, deps, fn, *args):
        jobs[name] = (cost, deps, functools.partial(fn, *args))

    for a in range(a_dev):
        job(("f", a), 2 * step, [], fill_bd, a)
        job(("p", a), 0, [("z", a)], fill_pick, a)
        job(("z", a), blocks * step // 2, [("f", a)], start_columns, a)
        if a >= turned_first:
            for c in range(blocks):
                job(("g", a, c), 9 * blocks * step // 4, [("z", a)], fold, a, c)
            job(("h", a), 0, [("g", a, c) for c in range(blocks)], gather, a)
            for r in range(blocks):
                job(("a", a, r), blocks * step, [("h", a)] + [("a", a, c) for c in range(r)], fold_a, a, r)
                job(("c", a, r), (blocks - r) * step, [("a", a, c) for c in range(r, blocks)], fold_b, a, r)
                job(("s", a, r), step, [("c", a, r), ("p", a)], scatter, a, r)
            continue
        for r in range(blocks):
            job(("a", a, r), blocks * step, [("z", a)] + [("ca", a, c) for c in range(r)], sweep_a, a, r)
            job(("ca", a, r), step // 2, [("a", a, r)], column_a, a, r)
            later = range(r + 1, blocks)
            job(("b", a, r), (blocks - r) * step, [("ca", a, r)] + [("cb", a, c) for c in later], sweep_b, a, r)
            job(("cb", a, r), step // 2, [("b", a, r)], column_b, a, r)
            job(("c", a, r), (r + 1) * step, [("cb", a, c) for c in range(r + 1)], sweep_c, a, r)
            job(("s", a, r), step, [("c", a, r), ("p", a)], scatter, a, r)
    for fn in in_order(jobs):
        fn()

    def send_acc(d):
        return pltpu.make_async_remote_copy(
            src_ref=acc.at[SPAN + d], dst_ref=landed.at[SPAN - d], send_sem=as_sem.at[SPAN - d],
            recv_sem=ar_sem.at[SPAN - d], device_id={"atom": atom_at(d)}, device_id_type=pl.DeviceIdType.MESH,
        )

    for p in range(places):
        acc[p] = whole[0][p * lm:(p + 1) * lm]
    a_copies = [send_acc(d) for d in shifts]
    for copy in a_copies:
        copy.start()
    r_copy.wait()
    own = diagonal(t_turned)
    for copy in a_copies:
        copy.wait()
    gathered = acc[SPAN]
    for d in shifts:
        gathered = gathered + landed[SPAN - d]
    high = gathered.astype(bf16)
    low = (gathered - high.astype(f32)).astype(bf16)
    received = t_turned + (mm(high, own) + mm(low, own))
    turned = mm(diagonal(received.astype(bf16).astype(f32)), r_v[...])
    products = turned * r_v[...].astype(f32)
    density = jnp.sum(products.reshape(a_dev, lm, products.shape[1]), axis=1) * w_ref[0]
    part = density.shape[1] // n_energy
    for q in range(n_energy):
        d_mine[q] = density[:, q * part:(q + 1) * part]

    def send_d(d):
        to = lax.rem(my_e + d, n_energy)
        return pltpu.make_async_remote_copy(
            src_ref=d_mine.at[to], dst_ref=d_land.at[d - 1], send_sem=ds_sem.at[d - 1],
            recv_sem=dr_sem.at[d - 1], device_id={"energy": to}, device_id_type=pl.DeviceIdType.MESH,
        )

    d_copies = [send_d(d) for d in range(1, n_energy)]
    for copy in d_copies:
        copy.start()
    for copy in d_copies:
        copy.wait()
    result = d_mine[my_e]
    for d in range(1, n_energy):
        result = result + d_land[d - 1]
    out_ref[...] = result


def shards(n_atom, n_energy, t_matrix, structure, radial, weights, neighbours, live):
    _, a_dev, lm, _ = t_matrix.shape
    zone = neighbours.shape[1]
    mesh_points = radial.shape[-1]
    dim, lanes, places = zone * lm, a_dev * lm, 2 * SPAN + 1
    share = mesh_points // n_energy
    vmem = pl.BlockSpec(memory_space=pltpu.VMEM)
    hbm = pl.BlockSpec(memory_space=pltpu.HBM)
    f32, bf16 = jnp.float32, jnp.bfloat16
    dma = pltpu.SemaphoreType.DMA
    pin = functools.partial(pltpu.with_memory_space_constraint, memory_space=pltpu.HBM)
    return pl.pallas_call(
        functools.partial(kernel, n_atom, n_energy, a_dev, lm, zone),
        out_shape=jax.ShapeDtypeStruct((a_dev, share), f32),
        in_specs=[hbm] * 6,
        out_specs=vmem,
        scratch_shapes=[
            pltpu.VMEM((lanes, lm), f32),
            pltpu.SMEM((1,), f32),
            pltpu.VMEM((a_dev, zone), jnp.int32),
            pltpu.VMEM((a_dev, zone), jnp.int32),
            pltpu.VMEM((a_dev, dim, dim), bf16),
            pltpu.VMEM((a_dev, dim, dim), bf16),
            pltpu.VMEM((lanes, mesh_points), bf16),
            pltpu.VMEM((lm, lanes), f32),
            pltpu.VMEM((places, lm, lanes), f32),
            pltpu.VMEM((a_dev, lm, lanes), f32),
            pltpu.VMEM((places * a_dev + 1, lm, lanes), bf16),
            pltpu.VMEM((places * a_dev + 1, lm, lanes), bf16),
            pltpu.VMEM((a_dev, dim // 2, 2 * lanes), bf16),
            pltpu.VMEM((a_dev, dim, lanes), bf16),
            pltpu.VMEM((a_dev, places, lm, dim), bf16),
            pltpu.VMEM((a_dev, lm, dim), f32),
            pltpu.VMEM((a_dev, 2 * lm, dim), bf16),
            pltpu.VMEM((a_dev, 2 * lm, dim), bf16),
            pltpu.VMEM((a_dev, lm, dim), bf16),
            pltpu.VMEM((a_dev, lm, dim), f32),
            pltpu.VMEM((a_dev, lm, dim), f32),
            pltpu.VMEM((a_dev * 3 // 8, dim // min(256, dim), lm, dim), f32),
            pltpu.VMEM((a_dev, zone), jnp.int32),
            pltpu.SMEM((a_dev, zone), jnp.int32),
            pltpu.VMEM((places, lm, lanes), f32),
            pltpu.VMEM((places, lm, lanes), f32),
            pltpu.VMEM((n_energy, a_dev, share), f32),
            pltpu.VMEM((n_energy, a_dev, share), f32),
            dma((a_dev,)),
            dma((6,)),
            dma((places,)),
            dma((places,)),
            dma((places,)),
            dma((places,)),
            dma((n_energy,)),
            dma((n_energy,)),
        ],
        compiler_params=pltpu.CompilerParams(collective_id=0, has_side_effects=True, vmem_limit_bytes=52 * 1024 * 1024),
        name="tau_density",
    )(
        pin(t_matrix.reshape(lanes, lm)),
        pin(structure.reshape(a_dev, dim, dim)),
        pin(radial.reshape(lanes, mesh_points)),
        weights,
        pin(neighbours),
        pin(live),
    )


def solution(mesh):
    in_specs = (
        P("energy", "atom", None, None),
        P("energy", "atom", None, None),
        P("energy", "atom", None, None),
        P("energy"),
        P("atom", None),
        P("atom", None),
    )
    out_specs = P("atom", "energy")
    body = functools.partial(shards, mesh.shape["atom"], mesh.shape["energy"])
    return jax.shard_map(body, mesh=mesh, in_specs=in_specs, out_specs=out_specs, check_vma=False)
```

```python
import functools

import jax
import jax.numpy as jnp
from jax import lax
from jax.experimental import pallas as pl
from jax.experimental.pallas import tpu as pltpu
from jax.sharding import PartitionSpec as P

ITERS = 4
SPAN = 3

NT = (((1,), (1,)), ((), ()))
NN = (((1,), (0,)), ((), ()))


def mm(a, b, dims=NN):
    return lax.dot_general(a, b, dims, preferred_element_type=jnp.float32)


WAIT = 300


def in_order(jobs):
    users = {name: [] for name in jobs}
    for name, (_, deps, _) in jobs.items():
        for dep in deps:
            users[dep].append(name)
    rank = {}

    def rank_of(name):
        if name not in rank:
            rank[name] = jobs[name][0] + max((WAIT + rank_of(user) for user in users[name]), default=0)
        return rank[name]

    order, ready_at, clock = [], {name: 0 for name in jobs if not jobs[name][1]}, 0
    missing = {name: len(deps) for name, (_, deps, _) in jobs.items()}
    at = {name: 0 for name in jobs}
    while ready_at:
        now = [name for name, t in ready_at.items() if t <= clock]
        if not now:
            clock = min(ready_at.values())
            continue
        name = max(now, key=rank_of)
        del ready_at[name]
        clock += jobs[name][0]
        order.append(jobs[name][2])
        for user in users[name]:
            at[user] = max(at[user], clock + WAIT)
            missing[user] -= 1
            if missing[user] == 0:
                ready_at[user] = at[user]
    return order


def kernel(
    n_atom, n_energy, a_dev, lm, zone,
    t_hbm, s_hbm, r_hbm, w_hbm, nb_hbm, live_hbm, out_ref,
    t_ref, w_ref, nb_ref, live_ref, s_v, s_t, r_v, t_send, t_all, firstx, table, hot, bd, pick, mask, reach, x12, x3, v, v3, v4, share,
    idx_v, idx_s, acc, landed, d_mine, d_land,
    s_sem, misc_sem, ts_sem, tr_sem, as_sem, ar_sem, ds_sem, dr_sem,
):
    bf16, f32 = jnp.bfloat16, jnp.float32
    places = 2 * SPAN + 1
    lanes = a_dev * lm
    dim = zone * lm
    per = lanes // lm
    me = lax.axis_index("atom")
    my_e = lax.axis_index("energy")

    small = [
        pltpu.make_async_copy(source, target, misc_sem.at[2 + n])
        for n, (source, target) in enumerate(
            ((t_hbm, t_ref), (nb_hbm, nb_ref), (live_hbm, live_ref), (w_hbm, w_ref))
        )
    ]
    for copy in small:
        copy.start()
    tile = min(256, dim)
    blocks = dim // tile
    s_copies = [pltpu.make_async_copy(s_hbm.at[a], s_v.at[a], s_sem.at[a]) for a in range(a_dev)]
    for copy in s_copies:
        copy.start(priority=1)
    r_copy = pltpu.make_async_copy(r_hbm, r_v, misc_sem.at[0])
    r_copy.start(priority=1)

    def atom_at(d):
        return lax.rem(me + (d + n_atom), n_atom)

    shifts = [s * d for d in range(SPAN, 0, -1) for s in (-1, 1)]
    barrier = pltpu.get_barrier_semaphore()
    for d in shifts:
        pl.semaphore_signal(barrier, inc=1, device_id={"atom": atom_at(d)}, device_id_type=pl.DeviceIdType.MESH)
    for d in range(1, n_energy):
        pl.semaphore_signal(
            barrier, inc=1, device_id={"energy": lax.rem(my_e + d, n_energy)}, device_id_type=pl.DeviceIdType.MESH
        )

    for copy in small:
        copy.wait()
    t_turned = jnp.transpose(t_ref[...])
    t_send[...] = t_turned
    ids = nb_ref[...] - (me - SPAN) * a_dev
    total = n_atom * a_dev
    ids = jnp.where(ids < 0, ids + total, ids)
    ids = jnp.where(ids >= total, ids - total, ids)
    ids = jnp.where(live_ref[...] > 0, ids, places * a_dev)
    idx_v[...] = ids
    i_copy = pltpu.make_async_copy(idx_v, idx_s, misc_sem.at[1])
    i_copy.start()

    lane16 = lax.broadcasted_iota(jnp.int32, (lm, lanes), 1)
    row16 = lax.broadcasted_iota(jnp.int32, (lm, lanes), 0)
    for a in range(a_dev):
        moved = t_turned if a == 0 else pltpu.roll(t_turned, lanes - a * lm, 1)
        firstx[a] = jnp.where(lane16 < lm, moved, 0.0)

    place_of = jnp.zeros(ids.shape, f32)
    for p in range(1, places + 1):
        place_of = place_of + jnp.where(ids >= p * a_dev, 1.0, 0.0)
    wide = lax.broadcasted_iota(jnp.int32, (zone, dim), 1)
    tall = lax.broadcasted_iota(jnp.int32, (zone, dim), 0)
    widen = jnp.where((wide >= tall * lm) & (wide < tall * lm + lm), 1.0, 0.0).astype(bf16)
    spread_place = mm(place_of.astype(bf16), widen)
    for a in range(a_dev):
        reach[a] = jnp.broadcast_to(spread_place[a:a + 1], (lm, dim))

    for n in range(a_dev):
        one = jnp.where(lane16 - row16 == n * lm, 1.0, 0.0).astype(bf16)
        for p in range(places):
            hot[p * a_dev + n] = one
    hot[places * a_dev] = jnp.zeros((lm, lanes), bf16)

    row = lax.broadcasted_iota(jnp.int32, (lanes, lanes), 0)
    col = lax.broadcasted_iota(jnp.int32, (lanes, lanes), 1)
    row_block, col_block = row // lm, col // lm
    same = row_block == col_block
    spread = jnp.where(row - row_block * lm == col - col_block * lm, 1.0, 0.0).astype(bf16)

    def diagonal(block):
        return jnp.where(same, jnp.concatenate([block] * a_dev, axis=0), 0.0).astype(bf16)

    unit = lax.broadcasted_iota(jnp.int32, (tile, tile), 0) == lax.broadcasted_iota(jnp.int32, (tile, tile), 1)
    unit = jnp.where(unit, 1.0, 0.0).astype(bf16)
    start = jnp.zeros((lm, tile - lanes), f32)

    def left_of(a, c):
        if c > 0:
            return unit
        return jnp.concatenate([unit, jnp.concatenate([firstx[a], start], axis=1).astype(bf16)], axis=0)

    def turn_tile(a, c, rows):
        got = mm(left_of(a, c), s_v[a, rows, c * tile:(c + 1) * tile], NT).astype(bf16)
        s_t[a, c * tile:(c + 1) * tile, rows] = got[:tile]
        if c == 0:
            v[a, :, rows] = got[tile:]

    def fill_pick(a):
        for s in range(zone):
            pick[a, pl.ds(s * lm, lm), :] = hot[idx_s[a, s]]

    def turn(a, carry):
        pltpu.make_async_copy(s_hbm.at[a], s_v.at[a], s_sem.at[a]).wait()
        for c in range(blocks):
            turn_tile(a, c, slice(0, dim))
        for p in range(places):
            mask[a, p] = jnp.where(reach[a] == p, 1.0, 0.0).astype(bf16)
        return carry

    early = a_dev // 4
    turned_first = a_dev - a_dev * 3 // 8
    lax.fori_loop(0, early, turn, 0)

    pl.semaphore_wait(barrier, len(shifts) + n_energy - 1)

    def send_t(d):
        return pltpu.make_async_remote_copy(
            src_ref=t_send, dst_ref=t_all.at[SPAN - d], send_sem=ts_sem.at[SPAN - d],
            recv_sem=tr_sem.at[SPAN - d], device_id={"atom": atom_at(d)}, device_id_type=pl.DeviceIdType.MESH,
        )

    t_copies = [send_t(d) for d in shifts]
    for copy in t_copies:
        copy.start()

    def begin(a, carry):
        pltpu.make_async_copy(s_hbm.at[a], s_v.at[a], s_sem.at[a]).wait()
        got = mm(firstx[a].astype(bf16), s_v[a, :, :lanes], NT)
        v4[a] = got
        v[a] = got.astype(bf16)
        for p in range(places):
            mask[a, p] = jnp.where(reach[a] == p, 1.0, 0.0).astype(bf16)
        return carry

    lax.fori_loop(early, turned_first, turn, 0)
    lax.fori_loop(turned_first, a_dev, begin, 0)
    i_copy.wait()

    def fill_table(place, block):
        block = mm(diagonal(block), spread).astype(bf16)
        table[pl.ds(place * a_dev, a_dev)] = block.reshape(a_dev, lm, lanes)

    fill_table(SPAN, t_turned)
    table[places * a_dev] = jnp.zeros((lm, lanes), bf16)
    for copy in t_copies:
        copy.wait()
    for d in shifts:
        fill_table(SPAN - d, t_all[SPAN - d])

    keep = [jnp.where(lane16 // lm == b, 1.0, 0.0).astype(bf16) for b in range(per)]

    def fill_bd(a):
        for s in range(zone):
            g = s // per
            at = g // 2 * lanes + s % per * lm
            half = slice(g % 2 * lanes, (g % 2 + 1) * lanes)
            bd[a, at:at + lm, half] = table[idx_s[a, s]] * keep[s % per]

    def column(a, r):
        halves = [slice(h * lanes, (h + 1) * lanes) for h in range(2)]
        left = jnp.concatenate([v[a, :, r * tile + h * lanes:r * tile + (h + 1) * lanes] for h in range(2)], axis=0)
        both = mm(left, bd[a, r * lanes:(r + 1) * lanes, :])
        parts = [both[h * lm:(h + 1) * lm, halves[h]] for h in range(2)]
        if r == 0:
            parts[0] = parts[0] + firstx[a]
        return jnp.concatenate([part.astype(bf16) for part in parts], axis=1)

    def cols(lo, hi):
        return slice(lo * tile, hi * tile)

    def start_columns(a):
        for r in range(blocks):
            x12[a, :lm, cols(r, r + 1)] = column(a, r)

    def sweep_a(a, r):
        here = cols(r, r + 1)
        got = mm(x12[a, :lm, cols(r, blocks)], s_t[a, cols(r, blocks), here])
        if r > 0:
            both = mm(x12[a, :, cols(0, r)], s_t[a, cols(0, r), here])
            got = got + both[:lm]
            v3[a, :, here] = both[lm:]
        v[a, :, here] = got.astype(bf16)

    def column_a(a, r):
        got = column(a, r)
        x12[a, lm:, cols(r, r + 1)] = got
        x3[a, :lm, cols(r, r + 1)] = got

    def sweep_b(a, r):
        here = cols(r, r + 1)
        got = mm(x3[a, :lm, cols(r, r + 1)], s_t[a, here, here])
        if r + 1 < blocks:
            both = mm(x3[a, :, cols(r + 1, blocks)], s_t[a, cols(r + 1, blocks), here])
            got = got + both[:lm]
            v4[a, :, here] = both[lm:]
        if r > 0:
            got = got + v3[a, :, here]
        v[a, :, here] = got.astype(bf16)

    def column_b(a, r):
        x3[a, lm:, cols(r, r + 1)] = column(a, r)

    def sweep_c(a, r):
        here = cols(r, r + 1)
        got = mm(x3[a, lm:, cols(0, r + 1)], s_t[a, cols(0, r + 1), here])
        if r + 1 < blocks:
            got = got + v4[a, :, here]
        v[a, :, here] = got.astype(bf16)

    void = jnp.zeros((lanes, lanes), bf16)

    def fold(a, c):
        rows = []
        for g in range(2):
            block = bd[a, c * lanes:(c + 1) * lanes, g * lanes:(g + 1) * lanes]
            rows.append(jnp.concatenate([block, void] if g == 0 else [void, block], axis=1))
        left = jnp.concatenate(rows + [x12[a, :lm, cols(c, c + 1)]], axis=0)
        got = mm(left, s_v[a, :, cols(c, c + 1)], NT)
        s_t[a, cols(c, c + 1), :] = got[:tile].astype(bf16)
        share[a - turned_first, c] = got[tile:]

    def gather(a):
        got = share[a - turned_first, 0]
        for c in range(1, blocks):
            got = got + share[a - turned_first, c]
        x12[a, :lm, :] = got.astype(bf16)

    def fold_a(a, r):
        here = cols(r, r + 1)
        got = mm(x12[a, :lm, cols(r, blocks)], s_t[a, cols(r, blocks), here]) + v4[a, :, here]
        if r > 0:
            both = mm(x12[a, :, cols(0, r)], s_t[a, cols(0, r), here])
            got = got + both[:lm]
            v3[a, :, here] = both[lm:]
        x12[a, lm:, here] = got.astype(bf16)
        x3[a, :lm, here] = got.astype(bf16)

    def fold_b(a, r):
        here = cols(r, r + 1)
        got = mm(x3[a, :lm, cols(r, blocks)], s_t[a, cols(r, blocks), here]) + v4[a, :, here]
        if r > 0:
            got = got + v3[a, :, here]
        v[a, :, here] = got.astype(bf16)

    whole = [None]

    def scatter(a, r):
        here = cols(r, r + 1)
        block = v[a, :, here]
        left = jnp.concatenate([block * mask[a, p, :, here] for p in range(places)], axis=0)
        got = mm(left, pick[a, here, :])
        whole[0] = got if whole[0] is None else whole[0] + got

    step = tile // 8
    jobs = {}

    def job(name, cost, deps, fn, *args):
        jobs[name] = (cost, deps, functools.partial(fn, *args))

    for a in range(a_dev):
        job(("f", a), 2 * step, [], fill_bd, a)
        job(("p", a), 0, [("z", a)], fill_pick, a)
        job(("z", a), blocks * step // 2, [("f", a)], start_columns, a)
        if a >= turned_first:
            for c in range(blocks):
                job(("g", a, c), 9 * blocks * step // 4, [("z", a)], fold, a, c)
            job(("h", a), 0, [("g", a, c) for c in range(blocks)], gather, a)
            for r in range(blocks):
                job(("a", a, r), blocks * step, [("h", a)] + [("a", a, c) for c in range(r)], fold_a, a, r)
                job(("c", a, r), (blocks - r) * step, [("a", a, c) for c in range(r, blocks)], fold_b, a, r)
                job(("s", a, r), step, [("c", a, r), ("p", a)], scatter, a, r)
            continue
        for r in range(blocks):
            job(("a", a, r), blocks * step, [("z", a)] + [("ca", a, c) for c in range(r)], sweep_a, a, r)
            job(("ca", a, r), step // 2, [("a", a, r)], column_a, a, r)
            later = range(r + 1, blocks)
            job(("b", a, r), (blocks - r) * step, [("ca", a, r)] + [("cb", a, c) for c in later], sweep_b, a, r)
            job(("cb", a, r), step // 2, [("b", a, r)], column_b, a, r)
            job(("c", a, r), (r + 1) * step, [("cb", a, c) for c in range(r + 1)], sweep_c, a, r)
            job(("s", a, r), step, [("c", a, r), ("p", a)], scatter, a, r)
    for fn in in_order(jobs):
        fn()

    def send_acc(d):
        return pltpu.make_async_remote_copy(
            src_ref=acc.at[SPAN + d], dst_ref=landed.at[SPAN - d], send_sem=as_sem.at[SPAN - d],
            recv_sem=ar_sem.at[SPAN - d], device_id={"atom": atom_at(d)}, device_id_type=pl.DeviceIdType.MESH,
        )

    for p in range(places):
        acc[p] = whole[0][p * lm:(p + 1) * lm]
    a_copies = [send_acc(d) for d in reversed(shifts)]
    for copy in a_copies:
        copy.start()
    r_copy.wait()
    own = diagonal(t_turned)
    for copy in a_copies:
        copy.wait()
    gathered = acc[SPAN]
    for d in shifts:
        gathered = gathered + landed[SPAN - d]
    high = gathered.astype(bf16)
    low = (gathered - high.astype(f32)).astype(bf16)
    received = t_turned + (mm(high, own) + mm(low, own))
    turned = mm(diagonal(received.astype(bf16).astype(f32)), r_v[...])
    products = turned * r_v[...].astype(f32)
    density = jnp.sum(products.reshape(a_dev, lm, products.shape[1]), axis=1) * w_ref[0]
    part = density.shape[1] // n_energy
    for q in range(n_energy):
        d_mine[q] = density[:, q * part:(q + 1) * part]

    def send_d(d):
        to = lax.rem(my_e + d, n_energy)
        return pltpu.make_async_remote_copy(
            src_ref=d_mine.at[to], dst_ref=d_land.at[d - 1], send_sem=ds_sem.at[d - 1],
            recv_sem=dr_sem.at[d - 1], device_id={"energy": to}, device_id_type=pl.DeviceIdType.MESH,
        )

    d_copies = [send_d(d) for d in range(1, n_energy)]
    for copy in d_copies:
        copy.start()
    for copy in d_copies:
        copy.wait()
    result = d_mine[my_e]
    for d in range(1, n_energy):
        result = result + d_land[d - 1]
    out_ref[...] = result


def shards(n_atom, n_energy, t_matrix, structure, radial, weights, neighbours, live):
    _, a_dev, lm, _ = t_matrix.shape
    zone = neighbours.shape[1]
    mesh_points = radial.shape[-1]
    dim, lanes, places = zone * lm, a_dev * lm, 2 * SPAN + 1
    share = mesh_points // n_energy
    vmem = pl.BlockSpec(memory_space=pltpu.VMEM)
    hbm = pl.BlockSpec(memory_space=pltpu.HBM)
    f32, bf16 = jnp.float32, jnp.bfloat16
    dma = pltpu.SemaphoreType.DMA
    pin = functools.partial(pltpu.with_memory_space_constraint, memory_space=pltpu.HBM)
    return pl.pallas_call(
        functools.partial(kernel, n_atom, n_energy, a_dev, lm, zone),
        out_shape=jax.ShapeDtypeStruct((a_dev, share), f32),
        in_specs=[hbm] * 6,
        out_specs=vmem,
        scratch_shapes=[
            pltpu.VMEM((lanes, lm), f32),
            pltpu.SMEM((1,), f32),
            pltpu.VMEM((a_dev, zone), jnp.int32),
            pltpu.VMEM((a_dev, zone), jnp.int32),
            pltpu.VMEM((a_dev, dim, dim), bf16),
            pltpu.VMEM((a_dev, dim, dim), bf16),
            pltpu.VMEM((lanes, mesh_points), bf16),
            pltpu.VMEM((lm, lanes), f32),
            pltpu.VMEM((places, lm, lanes), f32),
            pltpu.VMEM((a_dev, lm, lanes), f32),
            pltpu.VMEM((places * a_dev + 1, lm, lanes), bf16),
            pltpu.VMEM((places * a_dev + 1, lm, lanes), bf16),
            pltpu.VMEM((a_dev, dim // 2, 2 * lanes), bf16),
            pltpu.VMEM((a_dev, dim, lanes), bf16),
            pltpu.VMEM((a_dev, places, lm, dim), bf16),
            pltpu.VMEM((a_dev, lm, dim), f32),
            pltpu.VMEM((a_dev, 2 * lm, dim), bf16),
            pltpu.VMEM((a_dev, 2 * lm, dim), bf16),
            pltpu.VMEM((a_dev, lm, dim), bf16),
            pltpu.VMEM((a_dev, lm, dim), f32),
            pltpu.VMEM((a_dev, lm, dim), f32),
            pltpu.VMEM((a_dev * 3 // 8, dim // min(256, dim), lm, dim), f32),
            pltpu.VMEM((a_dev, zone), jnp.int32),
            pltpu.SMEM((a_dev, zone), jnp.int32),
            pltpu.VMEM((places, lm, lanes), f32),
            pltpu.VMEM((places, lm, lanes), f32),
            pltpu.VMEM((n_energy, a_dev, share), f32),
            pltpu.VMEM((n_energy, a_dev, share), f32),
            dma((a_dev,)),
            dma((6,)),
            dma((places,)),
            dma((places,)),
            dma((places,)),
            dma((places,)),
            dma((n_energy,)),
            dma((n_energy,)),
        ],
        compiler_params=pltpu.CompilerParams(collective_id=0, has_side_effects=True, vmem_limit_bytes=52 * 1024 * 1024),
        name="tau_density",
    )(
        pin(t_matrix.reshape(lanes, lm)),
        pin(structure.reshape(a_dev, dim, dim)),
        pin(radial.reshape(lanes, mesh_points)),
        weights,
        pin(neighbours),
        pin(live),
    )


def solution(mesh):
    in_specs = (
        P("energy", "atom", None, None),
        P("energy", "atom", None, None),
        P("energy", "atom", None, None),
        P("energy"),
        P("atom", None),
        P("atom", None),
    )
    out_specs = P("atom", "energy")
    body = functools.partial(shards, mesh.shape["atom"], mesh.shape["energy"])
    return jax.shard_map(body, mesh=mesh, in_specs=in_specs, out_specs=out_specs, check_vma=False)
```
